32 devices in a mesh: col: 16 (over z, y, x), row: 2 (over core).
Axes of the slice: x: 2, y: 2, z: 4, core: 2. Of those that a mesh axis runs over, the one named last changes fastest.
Arguments:
- kernel: float32 [512, 131072], P('row', 'col'), may hold values from -0.0234375 to 0.0234375
- slip_deficit: float32 [64, 131072], P(None, ('col', 'row')), may hold values from -6 to 6
- loading: float32 [512], P('row'), may hold values from -4 to 4
- direct_effect: float32 [512], P('row'), may hold values from 1 to 4
- log_state: float32 [64, 512], P(None, 'row'), may hold values from -1 to 1
Outputs:
- slip_rate: float32 [64, 512], P(None, 'row')
- next_state: float32 [64, 512], P(None, 'row')
The draws below stay inside these ranges and needn't reach their ends.
All inputs are finite; a program needn't handle non-finite values. Where the reference program divides by a largest or mean magnitude, that divisor is 1e-20 or more.
Results may differ from the reference program's by a relative error of at most 0.00013.
Values sent between devices are 32-bit elements; how exact they have to be, the bound alone decides.
A program may use at most 64 MiB of HBM per device.

```python
import math
import jax
import jax.numpy as jnp
from jax import lax

ROWS = 512
ENS = 64
PATCHES = 131072


def spiked(array, stream_key, source, target, parts, factor):
    owner, partner = [(jnp.arange(array.shape[position]) // (array.shape[position] // parts)).reshape([-1 if axis == position else 1 for axis in range(array.ndim)]) for position in (source, target)]
    chosen = jax.random.permutation(stream_key, parts)[partner]
    strong = (owner == chosen) | (owner == (partner + parts // 2) % parts)
    return jnp.where(strong, factor * array, array)


def levels(rng, shape, shards, least, top_value):
    loudness = 1.0
    for dim, blocks in shards:
        heights = jax.random.uniform(jax.random.fold_in(jax.random.fold_in(rng, 6), dim), (blocks,), jnp.float32, least / len(shards), top_value / len(shards))
        loudness = loudness * jnp.repeat(jnp.exp(heights), shape[dim] // blocks).reshape((-1,) + (1,) * (len(shape) - 1 - dim))
    return loudness


def noise(stream_key, extent, deviation, most, pieces=(), dtype=jnp.bfloat16):
    entries = jax.random.normal(stream_key, extent, jnp.float32) * deviation
    if len(pieces) > 0:
        entries = levels(stream_key, extent, pieces, -0.22, 0.18) * entries
    return jnp.clip(entries, min=-most, max=most).astype(dtype)


def bell_draw_with(own_key, extent, scale, reach, split, heavy, dtype=jnp.bfloat16):
    entries = scale * jax.random.normal(own_key, extent, jnp.float32)
    if split:
        entries = entries * levels(own_key, extent, split, -0.22, 0.18)
    return jnp.clip(spiked(entries, jax.random.fold_in(own_key, 3), *heavy), -reach, reach).astype(dtype)


def setup_inputs(seed: int = 0) -> dict:
    keys = jax.random.split(jax.random.key(seed), 6)
    return {
        "kernel": bell_draw_with(keys[0], (ROWS, PATCHES), PATCHES ** -0.5, 0.0234375, ((0, 2), (1, 16)), (1, 0, 16, 2.0), jnp.float32),
        "slip_deficit": noise(keys[1], (ENS, PATCHES), 1.0, 6.0, ((1, 32),), jnp.float32),
        "loading": noise(keys[2], (ROWS,), 1.0, 4.0, ((0, 2),), jnp.float32),
        "direct_effect": jnp.clip(jnp.exp(math.log(4.0) - 1.3862944 * jax.random.uniform(keys[3], (ROWS,), jnp.float32) ** levels(keys[3], (ROWS,), ((0, 2),), -0.2, 0.2)), 1.0, 4.0),
        "log_state": jnp.clip(jax.random.uniform(keys[4], (ENS, ROWS), jnp.float32, -1.0, 1.0) * levels(keys[4], (ENS, ROWS), ((1, 2),), -0.4, 0.0), -1.0, 1.0),
    }


def reference(kernel, slip_deficit, loading, direct_effect, log_state):
    stress = lax.dot_general(slip_deficit, kernel, (((1,), (1,)), ((), ())), precision=lax.Precision.HIGHEST, preferred_element_type=jnp.float32)
    stress = stress + loading[None, :]
    slip_rate = 2.0 * jnp.exp(-log_state) * jnp.sinh(stress / direct_effect[None, :])
    peak_rate = jnp.max(jnp.abs(slip_rate), axis=1) + 1e-6
    step_size = 1.0 / peak_rate
    next_state = log_state + step_size[:, None] * (jnp.exp(-log_state) - jnp.abs(slip_rate))
    return slip_rate, next_state
```

```python
import functools
import math

import jax
import jax.numpy as jnp
from jax import lax
from jax.experimental import pallas as pl
from jax.experimental.pallas import tpu as pltpu
from jax.sharding import PartitionSpec as P

MESH = pl.DeviceIdType.MESH
LANES = 128
LOG_HALF = math.log(0.5)


def sinh(x):
    square = x * x
    series = 1.0 / 362880.0
    for order in (5040.0, 120.0, 6.0, 1.0):
        series = series * square + 1.0 / order
    wide = jnp.exp(x + LOG_HALF) - jnp.exp(LOG_HALF - x)
    return jnp.where(jnp.abs(x) < 1.0, x * series, wide)


def split(x):
    high = x.astype(jnp.bfloat16)
    return high, (x - high.astype(jnp.float32)).astype(jnp.bfloat16)


def times_transposed(a, b):
    return lax.dot_general(a, b, (((1,), (1,)), ((), ())), preferred_element_type=jnp.float32)


def body(
    cols, rows, owners, chunk,
    kernel_hbm, slip_hbm, loading_hbm, effect_hbm, state_hbm,
    rate_ref, next_ref,
    kernel_buf, slip_buf, total, loading_all, effect_all, state_all,
    state_box, out_box, in_box, peak_out, peak_in, step_all,
    kernel_sem, slip_sem, swap_send, swap_recv, aux_sem, aux_send, aux_recv,
    sum_send, sum_recv, gather_send, gather_recv,
):
    n = cols * rows
    col, row = lax.axis_index("col"), lax.axis_index("row")
    me = col * rows + row
    members, width = state_hbm.shape
    share = members // owners
    half = slip_hbm.shape[1]
    pieces = half // chunk

    def place(target):
        return {"col": lax.div(target, rows), "row": lax.rem(target, rows)}

    barrier = pltpu.get_barrier_semaphore()

    def greet(k, carry):
        pl.semaphore_signal(barrier, inc=1, device_id=place(lax.rem(me + k, n)), device_id_type=MESH)
        return carry

    lax.fori_loop(1, n, greet, 0)

    for j in range(pieces):
        pltpu.make_async_copy(slip_hbm.at[:, pl.ds(j * chunk, chunk)], slip_buf.at[j], slip_sem.at[j]).start()
    extras = ((loading_hbm, loading_all), (effect_hbm, effect_all), (state_hbm, state_all))
    for i, (src, dst) in enumerate(extras):
        pltpu.make_async_copy(src, dst.at[0], aux_sem.at[i]).start()
    for h in range(rows):
        base = lax.rem(row + h, rows) * half
        for j in range(pieces):
            start = pl.multiple_of(base + j * chunk, chunk)
            pltpu.make_async_copy(kernel_hbm.at[:, pl.ds(start, chunk)], kernel_buf.at[h * pieces + j], kernel_sem.at[h * pieces + j]).start()

    def multiply(j):
        pltpu.make_async_copy(kernel_hbm.at[:, pl.ds(0, chunk)], kernel_buf.at[j], kernel_sem.at[j]).wait()
        slip_high, slip_low = split(slip_buf[j])
        kernel_high, kernel_low = split(kernel_buf[j])
        both = times_transposed(jnp.concatenate([slip_high, slip_low], axis=0), kernel_high)
        return both[:members] + both[members:] + times_transposed(slip_high, kernel_low)

    total[...] = jnp.zeros_like(total)

    def own(j, carry):
        pltpu.make_async_copy(slip_hbm.at[:, pl.ds(0, chunk)], slip_buf.at[j], slip_sem.at[j]).wait()
        total[...] += multiply(j)
        return carry

    lax.fori_loop(0, pieces, own, 0)

    for i, (src, dst) in enumerate(extras):
        pltpu.make_async_copy(src, dst.at[0], aux_sem.at[i]).wait()
    pl.semaphore_wait(barrier, n - 1)

    def swap(h, j):
        other = lax.rem(row + rows - h, rows)
        return pltpu.make_async_remote_copy(
            src_ref=slip_buf.at[j], dst_ref=slip_buf.at[h * pieces + j],
            send_sem=swap_send.at[h * pieces + j], recv_sem=swap_recv.at[h * pieces + j],
            device_id={"col": col, "row": other}, device_id_type=MESH)

    def aux(h):
        other = lax.rem(row + rows - h, rows)
        return [
            pltpu.make_async_remote_copy(
                src_ref=dst.at[0], dst_ref=dst.at[h], send_sem=aux_send.at[h, i], recv_sem=aux_recv.at[h, i],
                device_id={"col": col, "row": other}, device_id_type=MESH)
            for i, (src, dst) in enumerate(extras)
        ]

    for h in range(1, rows):
        for j in range(pieces):
            swap(h, j).start()
        for copy in aux(h):
            copy.start()

    for h in range(1, rows):
        def others(j, carry):
            swap(h, j).wait_recv()
            total[...] += multiply(h * pieces + j)
            return carry

        lax.fori_loop(0, pieces, others, 0)

    value = total[...]
    for o in range(owners):
        out_box[o] = value[o * share:(o + 1) * share]

    def send_sum(target):
        return pltpu.make_async_remote_copy(
            src_ref=out_box.at[target], dst_ref=in_box.at[me], send_sem=sum_send, recv_sem=sum_recv,
            device_id=place(target), device_id_type=MESH)

    def send_rate(target):
        return pltpu.make_async_remote_copy(
            src_ref=peak_out.at[lax.rem(target, rows)], dst_ref=peak_in.at[me], send_sem=gather_send, recv_sem=gather_recv,
            device_id=place(target), device_id_type=MESH)

    def when_owner(device, act):
        if owners == n:
            act()
        else:
            pl.when(device < owners)(act)

    def spread(k, carry):
        target = lax.rem(me + k, n)
        when_owner(target, lambda: send_sum(target).start())
        return carry

    lax.fori_loop(1, n, spread, 0)

    for h in range(1, rows):
        for copy in aux(h):
            copy.wait_recv()
    for h in range(rows):
        for o in range(owners):
            state_box[h, o] = state_all[h, o * share:(o + 1) * share]

    def finish_member_share():
        in_box[me] = out_box[me]
        blocks = in_box.at[pl.ds(0, n - 1)]
        pltpu.make_async_copy(blocks, blocks, sum_recv).wait()
        rates = []
        for q in range(rows):
            h = lax.rem(q - row + rows, rows)
            parts = [in_box[c * rows + q] for c in range(cols)]
            while len(parts) > 1:
                parts = [parts[i] + parts[i + 1] if i + 1 < len(parts) else parts[i] for i in range(0, len(parts), 2)]
            stress = parts[0] + loading_all[h]
            rates.append(2.0 * jnp.exp(-state_box[h, me]) * sinh(stress / effect_all[h]))
        peak = functools.reduce(jnp.maximum, [jnp.max(jnp.abs(rate), axis=1, keepdims=True) for rate in rates])
        step = jnp.broadcast_to(1.0 / (peak + 1e-6), (share, LANES))
        for q in range(rows):
            peak_out[q, :, :width] = rates[q]
            peak_out[q, :, width:] = step
        peak_in[me] = peak_out[row]

        def share_out(k, carry):
            send_rate(lax.rem(me + k, n)).start()
            return carry

        lax.fori_loop(1, n, share_out, 0)

    when_owner(me, finish_member_share)

    decay = jnp.exp(-state_all[0])

    def await_all(sem, box, sent):
        for count, condition in sent:
            def act():
                blocks = box.at[pl.ds(0, count)]
                pltpu.make_async_copy(blocks, blocks, sem).wait()
            if condition is None:
                act()
            else:
                pl.when(condition)(act)

    if owners == n:
        mine_or_not = [(n - 1, None)]
    else:
        mine_or_not = [(owners - 1, me < owners), (owners, me >= owners)]
    await_all(gather_recv, peak_in, mine_or_not)

    for o in range(owners):
        block = peak_in[o]
        rate_ref[o * share:(o + 1) * share, :] = block[:, :width]
        step_all[o * share:(o + 1) * share, :] = block[:, width:]
    rate = rate_ref[...]
    step = step_all[...]
    for w in range(0, width, LANES):
        lanes = slice(w, w + LANES)
        next_ref[:, lanes] = state_all[0, :, lanes] + step * (decay[:, lanes] - jnp.abs(rate[:, lanes]))

    await_all(sum_send, out_box, mine_or_not)
    if owners == n:
        await_all(gather_send, peak_in, [(n - 1, None)])
    else:
        def sent_all():
            def once(k, carry):
                send_rate(lax.rem(me + k, n)).wait_send()
                return carry
            lax.fori_loop(1, n, once, 0)
        pl.when(me < owners)(sent_all)
    for h in range(1, rows):
        for j in range(pieces):
            swap(h, j).wait_send()
        for copy in aux(h):
            copy.wait_send()


def solution(mesh):
    cols, rows = mesh.shape["col"], mesh.shape["row"]
    n = cols * rows

    def on_device(kernel, slip_deficit, loading, direct_effect, log_state):
        members, width = log_state.shape
        half = slip_deficit.shape[1]
        owners = max(d for d in range(1, min(n, members) + 1) if members % d == 0)
        share = members // owners
        chunk = math.gcd(half, 1024)
        pieces = half // chunk
        slots = rows * pieces
        f32 = jnp.float32
        vmem = pl.BlockSpec(memory_space=pltpu.VMEM)
        hbm = pl.BlockSpec(memory_space=pl.ANY)
        return pl.pallas_call(
            functools.partial(body, cols, rows, owners, chunk),
            out_shape=[jax.ShapeDtypeStruct((members, width), f32)] * 2,
            in_specs=[hbm] * 5,
            out_specs=[vmem, vmem],
            scratch_shapes=[
                pltpu.VMEM((slots, width, chunk), f32),
                pltpu.VMEM((slots, members, chunk), f32),
                pltpu.VMEM((members, width), f32),
                pltpu.VMEM((rows, 1, width), f32),
                pltpu.VMEM((rows, 1, width), f32),
                pltpu.VMEM((rows, members, width), f32),
                pltpu.VMEM((rows, owners, share, width), f32),
                pltpu.VMEM((owners, share, width), f32),
                pltpu.VMEM((n, share, width), f32),
                pltpu.VMEM((rows, share, width + LANES), f32),
                pltpu.VMEM((owners, share, width + LANES), f32),
                pltpu.VMEM((members, LANES), f32),
                pltpu.SemaphoreType.DMA((slots,)),
                pltpu.SemaphoreType.DMA((pieces,)),
                pltpu.SemaphoreType.DMA((slots,)),
                pltpu.SemaphoreType.DMA((slots,)),
                pltpu.SemaphoreType.DMA((3,)),
                pltpu.SemaphoreType.DMA((rows, 3)),
                pltpu.SemaphoreType.DMA((rows, 3)),
                pltpu.SemaphoreType.DMA,
                pltpu.SemaphoreType.DMA,
                pltpu.SemaphoreType.DMA,
                pltpu.SemaphoreType.DMA,
            ],
            compiler_params=pltpu.CompilerParams(
                collective_id=0, has_side_effects=True, vmem_limit_bytes=63 * 2**20
            ),
        )(kernel, slip_deficit, loading.reshape(1, -1), direct_effect.reshape(1, -1), log_state)

    return jax.shard_map(
        on_device,
        mesh=mesh,
        in_specs=(P("row", "col"), P(None, ("col", "row")), P("row"), P("row"), P(None, "row")),
        out_specs=(P(None, "row"), P(None, "row")),
        check_vma=False,
    )
```

```python
import functools
import math

import jax
import jax.numpy as jnp
from jax import lax
from jax.experimental import pallas as pl
from jax.experimental.pallas import tpu as pltpu
from jax.sharding import PartitionSpec as P

MESH = pl.DeviceIdType.MESH
LANES = 128
LOG_HALF = math.log(0.5)


def sinh(x):
    square = x * x
    series = 1.0 / 362880.0
    for order in (5040.0, 120.0, 6.0, 1.0):
        series = series * square + 1.0 / order
    wide = jnp.exp(x + LOG_HALF) - jnp.exp(LOG_HALF - x)
    return jnp.where(jnp.abs(x) < 1.0, x * series, wide)


def split(x):
    high = x.astype(jnp.bfloat16)
    return high, (x - high.astype(jnp.float32)).astype(jnp.bfloat16)


def times_transposed(a, b):
    return lax.dot_general(a, b, (((1,), (1,)), ((), ())), preferred_element_type=jnp.float32)


def body(
    cols, rows, owners, chunk,
    kernel_hbm, slip_hbm, loading_hbm, effect_hbm, state_hbm,
    rate_ref, next_ref,
    kernel_buf, slip_buf, total, loading_all, effect_all, state_all,
    state_box, out_box, in_box, peak_out, peak_in, step_all,
    kernel_sem, slip_sem, swap_send, swap_recv, aux_sem, aux_send, aux_recv,
    sum_send, sum_recv, gather_send, gather_recv, hello, ready,
):
    n = cols * rows
    col, row = lax.axis_index("col"), lax.axis_index("row")
    me = col * rows + row
    members, width = state_hbm.shape
    share = members // owners
    half = slip_hbm.shape[1]
    pieces = half // chunk

    def place(target):
        return {"col": lax.div(target, rows), "row": lax.rem(target, rows)}

    barrier = pltpu.get_barrier_semaphore()
    leads = row == 1

    @pl.when(leads)
    def _():
        pl.semaphore_signal(barrier, inc=1, device_id={"col": col, "row": 0}, device_id_type=MESH)

    for j in range(pieces):
        pltpu.make_async_copy(slip_hbm.at[:, pl.ds(j * chunk, chunk)], slip_buf.at[j], slip_sem.at[j]).start()
    extras = ((loading_hbm, loading_all), (effect_hbm, effect_all), (state_hbm, state_all))
    for i, (src, dst) in enumerate(extras):
        pltpu.make_async_copy(src, dst.at[0], aux_sem.at[i]).start()
    for h in range(rows):
        base = lax.rem(row + h, rows) * half
        for j in range(pieces):
            start = pl.multiple_of(base + j * chunk, chunk)
            pltpu.make_async_copy(kernel_hbm.at[:, pl.ds(start, chunk)], kernel_buf.at[h * pieces + j], kernel_sem.at[h * pieces + j]).start()

    def swap(h, j):
        other = lax.rem(row + rows - h, rows)
        return pltpu.make_async_remote_copy(
            src_ref=slip_buf.at[j], dst_ref=slip_buf.at[h * pieces + j],
            send_sem=swap_send.at[h * pieces + j], recv_sem=swap_recv.at[h * pieces + j],
            device_id={"col": col, "row": other}, device_id_type=MESH)

    def aux(h):
        other = lax.rem(row + rows - h, rows)
        return [
            pltpu.make_async_remote_copy(
                src_ref=dst.at[0], dst_ref=dst.at[h], send_sem=aux_send.at[h, i], recv_sem=aux_recv.at[h, i],
                device_id={"col": col, "row": other}, device_id_type=MESH)
            for i, (src, dst) in enumerate(extras)
        ]

    @pl.when(leads)
    def _():
        pl.semaphore_wait(hello, 1)

        def greet(k, carry):
            pl.semaphore_signal(barrier, inc=1, device_id={"col": lax.rem(col + k, cols), "row": 1}, device_id_type=MESH)
            return carry

        lax.fori_loop(1, cols, greet, 0)

    @pl.when(jnp.logical_not(leads))
    def _():
        pl.semaphore_wait(barrier, 1)
        pl.semaphore_signal(hello, inc=1, device_id={"col": col, "row": 1}, device_id_type=MESH)

    for j in range(pieces):
        pltpu.make_async_copy(slip_hbm.at[:, pl.ds(0, chunk)], slip_buf.at[j], slip_sem.at[j]).wait()
        for h in range(1, rows):
            swap(h, j).start()
    for i, (src, dst) in enumerate(extras):
        pltpu.make_async_copy(src, dst.at[0], aux_sem.at[i]).wait()
    for h in range(1, rows):
        for copy in aux(h):
            copy.start()

    def multiply(j):
        pltpu.make_async_copy(kernel_hbm.at[:, pl.ds(0, chunk)], kernel_buf.at[j], kernel_sem.at[j]).wait()
        slip_high, slip_low = split(slip_buf[j])
        kernel_high, kernel_low = split(kernel_buf[j])
        both = times_transposed(jnp.concatenate([slip_high, slip_low], axis=0), kernel_high)
        return both[:members] + both[members:] + times_transposed(slip_high, kernel_low)

    total[...] = jnp.zeros_like(total)

    def own(j, carry):
        total[...] += multiply(j)
        return carry

    lax.fori_loop(0, pieces, own, 0)


    for h in range(1, rows):
        def others(j, carry):
            swap(h, j).wait_recv()
            total[...] += multiply(h * pieces + j)
            return carry

        lax.fori_loop(0, pieces, others, 0)

    @pl.when(leads)
    def _():
        pl.semaphore_wait(barrier, cols - 1)
        pl.semaphore_signal(ready, inc=1, device_id={"col": col, "row": 0}, device_id_type=MESH)

    @pl.when(jnp.logical_not(leads))
    def _():
        pl.semaphore_wait(ready, 1)

    value = total[...]
    for o in range(owners):
        out_box[o] = value[o * share:(o + 1) * share]

    def send_sum(target):
        return pltpu.make_async_remote_copy(
            src_ref=out_box.at[target], dst_ref=in_box.at[me], send_sem=sum_send, recv_sem=sum_recv,
            device_id=place(target), device_id_type=MESH)

    def send_rate(target):
        return pltpu.make_async_remote_copy(
            src_ref=peak_out.at[lax.rem(target, rows)], dst_ref=peak_in.at[me], send_sem=gather_send, recv_sem=gather_recv,
            device_id=place(target), device_id_type=MESH)

    def when_owner(device, act):
        if owners == n:
            act()
        else:
            pl.when(device < owners)(act)

    def spread(k, carry):
        target = lax.rem(me + k, n)
        when_owner(target, lambda: send_sum(target).start())
        return carry

    lax.fori_loop(1, n, spread, 0)

    for h in range(1, rows):
        for copy in aux(h):
            copy.wait_recv()
    for h in range(rows):
        for o in range(owners):
            state_box[h, o] = state_all[h, o * share:(o + 1) * share]

    def finish_member_share():
        in_box[me] = out_box[me]
        blocks = in_box.at[pl.ds(0, n - 1)]
        pltpu.make_async_copy(blocks, blocks, sum_recv).wait()
        rates = []
        for q in range(rows):
            h = lax.rem(q - row + rows, rows)
            parts = [in_box[c * rows + q] for c in range(cols)]
            while len(parts) > 1:
                parts = [parts[i] + parts[i + 1] if i + 1 < len(parts) else parts[i] for i in range(0, len(parts), 2)]
            stress = parts[0] + loading_all[h]
            rates.append(2.0 * jnp.exp(-state_box[h, me]) * sinh(stress / effect_all[h]))
        peak = functools.reduce(jnp.maximum, [jnp.max(jnp.abs(rate), axis=1, keepdims=True) for rate in rates])
        step = jnp.broadcast_to(1.0 / (peak + 1e-6), (share, LANES))
        for q in range(rows):
            peak_out[q, :, :width] = rates[q]
            peak_out[q, :, width:] = step
        peak_in[me] = peak_out[row]

        def share_out(k, carry):
            send_rate(lax.rem(me + k, n)).start()
            return carry

        lax.fori_loop(1, n, share_out, 0)

    when_owner(me, finish_member_share)

    decay = jnp.exp(-state_all[0])

    def await_all(sem, box, sent):
        for count, condition in sent:
            def act():
                blocks = box.at[pl.ds(0, count)]
                pltpu.make_async_copy(blocks, blocks, sem).wait()
            if condition is None:
                act()
            else:
                pl.when(condition)(act)

    if owners == n:
        mine_or_not = [(n - 1, None)]
    else:
        mine_or_not = [(owners - 1, me < owners), (owners, me >= owners)]
    await_all(gather_recv, peak_in, mine_or_not)

    for o in range(owners):
        block = peak_in[o]
        rate_ref[o * share:(o + 1) * share, :] = block[:, :width]
        step_all[o * share:(o + 1) * share, :] = block[:, width:]
    rate = rate_ref[...]
    step = step_all[...]
    for w in range(0, width, LANES):
        lanes = slice(w, w + LANES)
        next_ref[:, lanes] = state_all[0, :, lanes] + step * (decay[:, lanes] - jnp.abs(rate[:, lanes]))

    await_all(sum_send, out_box, mine_or_not)
    if owners == n:
        await_all(gather_send, peak_in, [(n - 1, None)])
    else:
        def sent_all():
            def once(k, carry):
                send_rate(lax.rem(me + k, n)).wait_send()
                return carry
            lax.fori_loop(1, n, once, 0)
        pl.when(me < owners)(sent_all)
    for h in range(1, rows):
        for j in range(pieces):
            swap(h, j).wait_send()
        for copy in aux(h):
            copy.wait_send()


def write_out(rate_vmem, next_vmem, rate_hbm, next_hbm, sem):
    copies = [
        pltpu.make_async_copy(src, dst, sem.at[i])
        for i, (src, dst) in enumerate(((rate_vmem, rate_hbm), (next_vmem, next_hbm)))
    ]
    for copy in copies:
        copy.start()
    for copy in copies:
        copy.wait()


def solution(mesh):
    cols, rows = mesh.shape["col"], mesh.shape["row"]
    n = cols * rows

    def on_device(kernel, slip_deficit, loading, direct_effect, log_state):
        members, width = log_state.shape
        half = slip_deficit.shape[1]
        owners = max(d for d in range(1, min(n, members) + 1) if members % d == 0)
        share = members // owners
        chunk = math.gcd(half, 1024)
        pieces = half // chunk
        slots = rows * pieces
        f32 = jnp.float32
        vmem = pl.BlockSpec(memory_space=pltpu.VMEM)
        hbm = pl.BlockSpec(memory_space=pltpu.HBM)
        results = [jax.ShapeDtypeStruct((members, width), f32)] * 2
        held = pl.pallas_call(
            functools.partial(body, cols, rows, owners, chunk),
            out_shape=[pltpu.VMEM((members, width), f32)] * 2,
            in_specs=[hbm] * 5,
            out_specs=[vmem, vmem],
            scratch_shapes=[
                pltpu.VMEM((slots, width, chunk), f32),
                pltpu.VMEM((slots, members, chunk), f32),
                pltpu.VMEM((members, width), f32),
                pltpu.VMEM((rows, 1, width), f32),
                pltpu.VMEM((rows, 1, width), f32),
                pltpu.VMEM((rows, members, width), f32),
                pltpu.VMEM((rows, owners, share, width), f32),
                pltpu.VMEM((owners, share, width), f32),
                pltpu.VMEM((n, share, width), f32),
                pltpu.VMEM((rows, share, width + LANES), f32),
                pltpu.VMEM((owners, share, width + LANES), f32),
                pltpu.VMEM((members, LANES), f32),
                pltpu.SemaphoreType.DMA((slots,)),
                pltpu.SemaphoreType.DMA((pieces,)),
                pltpu.SemaphoreType.DMA((slots,)),
                pltpu.SemaphoreType.DMA((slots,)),
                pltpu.SemaphoreType.DMA((3,)),
                pltpu.SemaphoreType.DMA((rows, 3)),
                pltpu.SemaphoreType.DMA((rows, 3)),
                pltpu.SemaphoreType.DMA,
                pltpu.SemaphoreType.DMA,
                pltpu.SemaphoreType.DMA,
                pltpu.SemaphoreType.DMA,
                pltpu.SemaphoreType.REGULAR,
                pltpu.SemaphoreType.REGULAR,
            ],
            compiler_params=pltpu.CompilerParams(
                collective_id=0, has_side_effects=True, vmem_limit_bytes=20 * 2**20
            ),
        )(*(pltpu.with_memory_space_constraint(x, pltpu.HBM) for x in (kernel, slip_deficit, loading.reshape(1, -1), direct_effect.reshape(1, -1), log_state)))
        return pl.pallas_call(
            write_out,
            out_shape=results,
            in_specs=[vmem] * 2,
            out_specs=[hbm] * 2,
            scratch_shapes=[pltpu.SemaphoreType.DMA((2,))],
            compiler_params=pltpu.CompilerParams(vmem_limit_bytes=2**20),
        )(*held)

    return jax.shard_map(
        on_device,
        mesh=mesh,
        in_specs=(P("row", "col"), P(None, ("col", "row")), P("row"), P("row"), P(None, "row")),
        out_specs=(P(None, "row"), P(None, "row")),
        check_vma=False,
    )
```

```python
import functools
import math

import jax
import jax.numpy as jnp
from jax import lax
from jax.experimental import pallas as pl
from jax.experimental.pallas import tpu as pltpu
from jax.sharding import PartitionSpec as P

MESH = pl.DeviceIdType.MESH
LANES = 128
LOG_HALF = math.log(0.5)


def sinh(x):
    square = x * x
    series = 1.0 / 362880.0
    for order in (5040.0, 120.0, 6.0, 1.0):
        series = series * square + 1.0 / order
    wide = jnp.exp(x + LOG_HALF) - jnp.exp(LOG_HALF - x)
    return jnp.where(jnp.abs(x) < 1.0, x * series, wide)


def split(x):
    high = x.astype(jnp.bfloat16)
    return high, (x - high.astype(jnp.float32)).astype(jnp.bfloat16)


def times_transposed(a, b):
    return lax.dot_general(a, b, (((1,), (1,)), ((), ())), preferred_element_type=jnp.float32)


def body(
    cols, rows, owners, chunk,
    kernel_hbm, slip_hbm, loading_hbm, effect_hbm, state_hbm,
    rate_ref, next_ref,
    kernel_buf, slip_buf, total, loading_all, effect_all, state_all,
    state_box, out_box, in_box, peak_out, peak_in, step_all,
    kernel_sem, slip_sem, swap_send, swap_recv, aux_sem, aux_send, aux_recv,
    sum_send, sum_recv, gather_send, gather_recv, hello, ready,
):
    n = cols * rows
    col, row = lax.axis_index("col"), lax.axis_index("row")
    me = col * rows + row
    members, width = state_hbm.shape
    share = members // owners
    half = slip_hbm.shape[1]
    pieces = half // chunk

    def place(target):
        return {"col": lax.div(target, rows), "row": lax.rem(target, rows)}

    barrier = pltpu.get_barrier_semaphore()
    leads = row == 1

    @pl.when(leads)
    def _():
        pl.semaphore_signal(barrier, inc=1, device_id={"col": col, "row": 0}, device_id_type=MESH)

    for j in range(pieces):
        pltpu.make_async_copy(slip_hbm.at[:, pl.ds(j * chunk, chunk)], slip_buf.at[j], slip_sem.at[j]).start()
    extras = ((loading_hbm, loading_all), (effect_hbm, effect_all), (state_hbm, state_all))
    for i, (src, dst) in enumerate(extras):
        pltpu.make_async_copy(src, dst.at[0], aux_sem.at[i]).start()
    for h in range(rows):
        base = lax.rem(row + h, rows) * half
        for j in range(pieces):
            start = pl.multiple_of(base + j * chunk, chunk)
            pltpu.make_async_copy(kernel_hbm.at[:, pl.ds(start, chunk)], kernel_buf.at[h * pieces + j], kernel_sem.at[h * pieces + j]).start()

    def swap(h, j):
        other = lax.rem(row + rows - h, rows)
        return pltpu.make_async_remote_copy(
            src_ref=slip_buf.at[j], dst_ref=slip_buf.at[h * pieces + j],
            send_sem=swap_send.at[h * pieces + j], recv_sem=swap_recv.at[h * pieces + j],
            device_id={"col": col, "row": other}, device_id_type=MESH)

    def aux(h):
        other = lax.rem(row + rows - h, rows)
        return [
            pltpu.make_async_remote_copy(
                src_ref=dst.at[0], dst_ref=dst.at[h], send_sem=aux_send.at[h, i], recv_sem=aux_recv.at[h, i],
                device_id={"col": col, "row": other}, device_id_type=MESH)
            for i, (src, dst) in enumerate(extras)
        ]

    @pl.when(leads)
    def _():
        pl.semaphore_wait(hello, 1)

        def greet(k, carry):
            pl.semaphore_signal(barrier, inc=1, device_id={"col": lax.rem(col + k, cols), "row": 1}, device_id_type=MESH)
            return carry

        lax.fori_loop(1, cols, greet, 0)

    @pl.when(jnp.logical_not(leads))
    def _():
        pl.semaphore_wait(barrier, 1)
        pl.semaphore_signal(hello, inc=1, device_id={"col": col, "row": 1}, device_id_type=MESH)

    for j in range(pieces):
        pltpu.make_async_copy(slip_hbm.at[:, pl.ds(0, chunk)], slip_buf.at[j], slip_sem.at[j]).wait()
        for h in range(1, rows):
            swap(h, j).start()
    for i, (src, dst) in enumerate(extras):
        pltpu.make_async_copy(src, dst.at[0], aux_sem.at[i]).wait()
    for h in range(1, rows):
        for copy in aux(h):
            copy.start()

    def multiply(j):
        pltpu.make_async_copy(kernel_hbm.at[:, pl.ds(0, chunk)], kernel_buf.at[j], kernel_sem.at[j]).wait()
        slip_high, slip_low = split(slip_buf[j])
        kernel_high, kernel_low = split(kernel_buf[j])
        both = times_transposed(jnp.concatenate([slip_high, slip_low], axis=0), kernel_high)
        return both[:members] + both[members:] + times_transposed(slip_high, kernel_low)

    total[...] = jnp.zeros_like(total)

    def own(j, carry):
        total[...] += multiply(j)
        return carry

    lax.fori_loop(0, pieces, own, 0)


    for h in range(1, rows):
        def others(j, carry):
            swap(h, j).wait_recv()
            total[...] += multiply(h * pieces + j)
            return carry

        lax.fori_loop(0, pieces, others, 0)

    @pl.when(leads)
    def _():
        pl.semaphore_wait(barrier, cols - 1)
        pl.semaphore_signal(ready, inc=1, device_id={"col": col, "row": 0}, device_id_type=MESH)

    @pl.when(jnp.logical_not(leads))
    def _():
        pl.semaphore_wait(ready, 1)

    value = total[...]
    for o in range(owners):
        out_box[o] = value[o * share:(o + 1) * share]

    def send_sum(target):
        return pltpu.make_async_remote_copy(
            src_ref=out_box.at[target], dst_ref=in_box.at[me], send_sem=sum_send, recv_sem=sum_recv,
            device_id=place(target), device_id_type=MESH)

    def send_rate(target):
        return pltpu.make_async_remote_copy(
            src_ref=peak_out.at[lax.rem(target, rows)], dst_ref=peak_in.at[me], send_sem=gather_send, recv_sem=gather_recv,
            device_id=place(target), device_id_type=MESH)

    def when_owner(device, act):
        if owners == n:
            act()
        else:
            pl.when(device < owners)(act)

    def spread(k, carry):
        target = lax.rem(me + k, n)
        when_owner(target, lambda: send_sum(target).start())
        return carry

    lax.fori_loop(1, n, spread, 0)

    for h in range(1, rows):
        for copy in aux(h):
            copy.wait_recv()
    for h in range(rows):
        for o in range(owners):
            state_box[h, o] = state_all[h, o * share:(o + 1) * share]

    def finish_member_share():
        in_box[me] = out_box[me]
        blocks = in_box.at[pl.ds(0, n - 1)]
        pltpu.make_async_copy(blocks, blocks, sum_recv).wait()
        rates = []
        for q in range(rows):
            h = lax.rem(q - row + rows, rows)
            parts = [in_box[c * rows + q] for c in range(cols)]
            while len(parts) > 1:
                parts = [parts[i] + parts[i + 1] if i + 1 < len(parts) else parts[i] for i in range(0, len(parts), 2)]
            stress = parts[0] + loading_all[h]
            rates.append(2.0 * jnp.exp(-state_box[h, me]) * sinh(stress / effect_all[h]))
        peak = functools.reduce(jnp.maximum, [jnp.max(jnp.abs(rate), axis=1, keepdims=True) for rate in rates])
        step = jnp.broadcast_to(1.0 / (peak + 1e-6), (share, LANES))
        for q in range(rows):
            peak_out[q, :, :width] = rates[q]
            peak_out[q, :, width:] = step
        peak_in[me] = peak_out[row]

        def share_out(k, carry):
            send_rate(lax.rem(me + k, n)).start()
            return carry

        lax.fori_loop(1, n, share_out, 0)

    when_owner(me, finish_member_share)

    decay = jnp.exp(-state_all[0])

    def await_all(sem, box, sent):
        for count, condition in sent:
            def act():
                blocks = box.at[pl.ds(0, count)]
                pltpu.make_async_copy(blocks, blocks, sem).wait()
            if condition is None:
                act()
            else:
                pl.when(condition)(act)

    if owners == n:
        mine_or_not = [(n - 1, None)]
    else:
        mine_or_not = [(owners - 1, me < owners), (owners, me >= owners)]
    await_all(gather_recv, peak_in, mine_or_not)

    for o in range(owners):
        block = peak_in[o]
        rate_ref[o * share:(o + 1) * share, :] = block[:, :width]
        step_all[o * share:(o + 1) * share, :] = block[:, width:]
    rate = rate_ref[...]
    step = step_all[...]
    for w in range(0, width, LANES):
        lanes = slice(w, w + LANES)
        next_ref[:, lanes] = state_all[0, :, lanes] + step * (decay[:, lanes] - jnp.abs(rate[:, lanes]))

    await_all(sum_send, out_box, mine_or_not)
    if owners == n:
        await_all(gather_send, peak_in, [(n - 1, None)])
    else:
        def sent_all():
            def once(k, carry):
                send_rate(lax.rem(me + k, n)).wait_send()
                return carry
            lax.fori_loop(1, n, once, 0)
        pl.when(me < owners)(sent_all)
    for h in range(1, rows):
        for j in range(pieces):
            swap(h, j).wait_send()
        for copy in aux(h):
            copy.wait_send()


def write_out(rate_vmem, next_vmem, rate_hbm, next_hbm, sem):
    copies = [
        pltpu.make_async_copy(src, dst, sem.at[i])
        for i, (src, dst) in enumerate(((rate_vmem, rate_hbm), (next_vmem, next_hbm)))
    ]
    for copy in copies:
        copy.start()
    for copy in copies:
        copy.wait()


def solution(mesh):
    cols, rows = mesh.shape["col"], mesh.shape["row"]
    n = cols * rows

    def on_device(kernel, slip_deficit, loading, direct_effect, log_state):
        members, width = log_state.shape
        half = slip_deficit.shape[1]
        owners = max(d for d in range(1, min(n, members) + 1) if members % d == 0)
        share = members // owners
        chunk = math.gcd(half, 2048)
        pieces = half // chunk
        slots = rows * pieces
        f32 = jnp.float32
        vmem = pl.BlockSpec(memory_space=pltpu.VMEM)
        hbm = pl.BlockSpec(memory_space=pltpu.HBM)
        results = [jax.ShapeDtypeStruct((members, width), f32)] * 2
        held = pl.pallas_call(
            functools.partial(body, cols, rows, owners, chunk),
            out_shape=[pltpu.VMEM((members, width), f32)] * 2,
            in_specs=[hbm] * 5,
            out_specs=[vmem, vmem],
            scratch_shapes=[
                pltpu.VMEM((slots, width, chunk), f32),
                pltpu.VMEM((slots, members, chunk), f32),
                pltpu.VMEM((members, width), f32),
                pltpu.VMEM((rows, 1, width), f32),
                pltpu.VMEM((rows, 1, width), f32),
                pltpu.VMEM((rows, members, width), f32),
                pltpu.VMEM((rows, owners, share, width), f32),
                pltpu.VMEM((owners, share, width), f32),
                pltpu.VMEM((n, share, width), f32),
                pltpu.VMEM((rows, share, width + LANES), f32),
                pltpu.VMEM((owners, share, width + LANES), f32),
                pltpu.VMEM((members, LANES), f32),
                pltpu.SemaphoreType.DMA((slots,)),
                pltpu.SemaphoreType.DMA((pieces,)),
                pltpu.SemaphoreType.DMA((slots,)),
                pltpu.SemaphoreType.DMA((slots,)),
                pltpu.SemaphoreType.DMA((3,)),
                pltpu.SemaphoreType.DMA((rows, 3)),
                pltpu.SemaphoreType.DMA((rows, 3)),
                pltpu.SemaphoreType.DMA,
                pltpu.SemaphoreType.DMA,
                pltpu.SemaphoreType.DMA,
                pltpu.SemaphoreType.DMA,
                pltpu.SemaphoreType.REGULAR,
                pltpu.SemaphoreType.REGULAR,
            ],
            compiler_params=pltpu.CompilerParams(
                collective_id=0, has_side_effects=True, vmem_limit_bytes=20 * 2**20
            ),
        )(*(pltpu.with_memory_space_constraint(x, pltpu.HBM) for x in (kernel, slip_deficit, loading.reshape(1, -1), direct_effect.reshape(1, -1), log_state)))
        return pl.pallas_call(
            write_out,
            out_shape=results,
            in_specs=[vmem] * 2,
            out_specs=[hbm] * 2,
            scratch_shapes=[pltpu.SemaphoreType.DMA((2,))],
            compiler_params=pltpu.CompilerParams(vmem_limit_bytes=2**20),
        )(*held)

    return jax.shard_map(
        on_device,
        mesh=mesh,
        in_specs=(P("row", "col"), P(None, ("col", "row")), P("row"), P("row"), P(None, "row")),
        out_specs=(P(None, "row"), P(None, "row")),
        check_vma=False,
    )
```
